32 devices in a mesh: section: 4 (over y, core), tensor: 4 (over z), dp: 2 (over x).
Axes of the slice: x: 2, y: 2, z: 4, core: 2. Of those that a mesh axis runs over, the one named last changes fastest.
Arguments:
- section_up: bfloat16 [4, 4096, 7168], P('section', 'dp', 'tensor'), may hold values from -0.09375 to 0.09375
- section_down: bfloat16 [4, 4096, 7168], P('section', 'dp', 'tensor'), may hold values from -0.0625 to 0.0625
- backup_up: bfloat16 [2, 4, 4, 128, 7168], P('dp', 'section', 'tensor'), may hold values from -0.09375 to 0.09375
- backup_down: bfloat16 [2, 4, 4, 128, 7168], P('dp', 'section', 'tensor'), may hold values from -0.0625 to 0.0625
- norm_gain: float32 [4, 4096], P('section'), may hold values from 0.25 to 1.75
- micro_batches: bfloat16 [4, 64, 4096], P(None, 'dp', 'tensor'), may hold values from -24 to 24
- failed_section: int32 [1], replicated, may hold values from 0 to 262143
- live_batches: int32 [1], replicated, may hold values from 0 to 196607
Outputs:
- finals: bfloat16 [4, 64, 4096], P('section', 'dp', 'tensor')
The draws below stay inside these ranges and needn't reach their ends.
Inputs may be any that keep to these rules, and one draw needn't show every extreme that they name: failed_section modulo the number of sections names the failed section. micro-batches 0 to 4 // 2 + (live_batches modulo (4 - 4 // 2 + 1)) - 1 run.
All inputs are finite; a program needn't handle non-finite values.
Results may differ from the reference program's by a relative error of at most 0.03.
Values may be sent and summed in bfloat16 or wider, within the bound.
A program may use at most 192 MiB of HBM per device.

```python
import math
import jax
import jax.numpy as jnp
from jax import lax

D = 4096
FF = 7168
MB = 4
TOKENS_MB = 64
ROWS_PIECE = 128
N_SECTION = 4
N_TENSOR = 4
N_DP = 2


def draw_micro_batches(key, part):
    first, second, third = jax.random.split(key, 3)
    shape = (MB, TOKENS_MB, D)
    row_scale = jnp.exp(jax.random.uniform(second, (MB, TOKENS_MB, 1), jnp.float32, math.log(0.3), math.log(3.0)))
    column_scale = jnp.exp(jax.random.uniform(third, (1, 1, D), jnp.float32, math.log(0.3), math.log(3.0)))
    values = jax.random.normal(first, shape, jnp.float32) * row_scale * column_scale
    return jnp.clip(values, -24.0, 24.0).astype(jnp.bfloat16)


def shard_levels(rng, extent, pieces, smallest, top_value):
    factor_of = 1.0
    for dim, shards_of in pieces:
        draws = jax.random.uniform(jax.random.fold_in(jax.random.fold_in(rng, 6), dim), (shards_of,), jnp.float32, smallest / len(pieces), top_value / len(pieces))
        factor_of = factor_of * jnp.repeat(jnp.exp(draws), extent[dim] // shards_of).reshape((-1,) + (1,) * (len(extent) - 1 - dim))
    return factor_of


def gaussian(key, shape, deviation, limit, shards=(), kind=jnp.bfloat16):
    entries = jax.random.normal(key, shape, jnp.float32) * deviation
    if len(shards) > 0:
        entries = shard_levels(key, shape, shards, -0.22, 0.18) * entries
    return jnp.clip(entries, min=-limit, max=limit).astype(kind)


def setup_inputs(seed: int = 0) -> dict:
    key_of = jax.random.split(jax.random.key(seed), 9)
    section_up = gaussian(key_of[0], (N_SECTION, D, FF), D ** -0.5, 0.09375, ((0, 4), (1, 2), (2, 4)))
    section_down = gaussian(key_of[1], (N_SECTION, D, FF), FF ** -0.5, 0.0625, ((0, 4), (1, 2), (2, 4)))
    backup_up = gaussian(key_of[2], (N_DP, N_SECTION, N_TENSOR, ROWS_PIECE, FF), D ** -0.5, 0.09375, ((0, 2), (1, 4), (2, 4)))
    backup_down = gaussian(key_of[3], (N_DP, N_SECTION, N_TENSOR, ROWS_PIECE, FF), FF ** -0.5, 0.0625, ((0, 2), (1, 4), (2, 4)))
    norm_gain = jnp.clip(1.0 + 0.15 * jax.random.normal(key_of[4], (N_SECTION, D), jnp.float32), 0.25, 1.75)
    micro_batches = draw_micro_batches(jax.random.fold_in(key_of[8], 71), 0)
    failed_section = jax.random.randint(key_of[6], (1,), 0, N_SECTION * 65536).astype(jnp.int32)
    live_batches = jax.random.randint(key_of[7], (1,), 0, 65536 * (MB - MB // 2 + 1)).astype(jnp.int32)
    return dict(section_up=section_up, section_down=section_down, backup_up=backup_up, backup_down=backup_down, norm_gain=norm_gain, micro_batches=micro_batches, failed_section=failed_section, live_batches=live_batches)


def reference(section_up, section_down, backup_up, backup_down, norm_gain, micro_batches, failed_section, live_batches):
    failed = failed_section[0] % N_SECTION
    live_count = MB // 2 + live_batches[0] % (MB - MB // 2 + 1)
    spare_up = backup_up.reshape(D, FF)
    spare_down = backup_down.reshape(D, FF)
    batch_index = lax.broadcasted_iota(jnp.int32, (MB, 1, 1), 0)
    inputs = jnp.where(batch_index < live_count, micro_batches, jnp.zeros_like(micro_batches))
    state_rows = inputs.reshape(MB * TOKENS_MB, D)
    block_width = FF // N_TENSOR

    def one_section(carried, section_layer):
        up_weight, down_weight, gain_row, section_index = section_layer
        chosen_up = jnp.where(section_index == failed, spare_up, up_weight)
        chosen_down = jnp.where(section_index == failed, spare_down, down_weight)
        values = carried.astype(jnp.float32)
        mean_square = lax.optimization_barrier(jnp.mean(values * values, axis=1, keepdims=True))
        normed = (values * lax.rsqrt(mean_square + 1e-05) * gain_row).astype(jnp.bfloat16)
        hidden = jax.nn.silu(jnp.dot(normed, chosen_up, preferred_element_type=jnp.float32)).astype(jnp.bfloat16)
        down_total = jnp.zeros((carried.shape[0], D), jnp.float32)
        for block_index in range(N_TENSOR):
            lower = block_index * block_width
            block_term = lax.dot_general(hidden[:, lower:lower + block_width], chosen_down[:, lower:lower + block_width], (((1,), (1,)), ((), ())), preferred_element_type=jnp.float32)
            down_total = down_total + lax.optimization_barrier(block_term.astype(jnp.bfloat16)).astype(jnp.float32)
        return ((values + down_total).astype(jnp.bfloat16), None)
    indices = jnp.arange(N_SECTION, dtype=jnp.int32)
    final_rows, _ = lax.scan(one_section, state_rows, (section_up, section_down, norm_gain, indices))
    return final_rows.reshape(MB, TOKENS_MB, D)
```

```python
import functools

import jax
import jax.numpy as jnp
from jax import lax
from jax.experimental import pallas as pl
from jax.experimental.pallas import tpu as pltpu
from jax.sharding import PartitionSpec as P

MESH = pl.DeviceIdType.MESH


def relay_kernel(
    sizes,
    failed,
    inputs_ref,
    gain_ref,
    up_hbm,
    down_hbm,
    spare_up,
    spare_down,
    finals_ref,
    up,
    down,
    xbuf,
    part_out,
    part_in,
    square_out,
    square_in,
    down_out,
    down_in,
    done_buf,
    fin,
    staged,
    weight_sem,
    spread_send,
    spread_recv,
    piece_send,
    piece_recv,
    start_send,
    start_recv,
    x_send,
    x_recv,
    part_send,
    part_recv,
    square_send,
    square_recv,
    down_send,
    down_recv,
    fin_send,
    fin_recv,
):
    S, T, R, chunks, group, tok = sizes
    s, t, d = lax.axis_index("section"), lax.axis_index("tensor"), lax.axis_index("dp")
    rows = group * R * tok
    width = xbuf.shape[-1]
    model = width * T * R
    first, last = s == 0, s == S - 1
    per_section = finals_ref.shape[0]

    is_failed = s == failed
    up_copy = pltpu.make_async_copy(up_hbm, up, weight_sem.at[0])
    down_copy = pltpu.make_async_copy(down_hbm, down, weight_sem.at[1])
    spares, chosen = (spare_up, spare_down), (up, down)
    piece, wide = spare_up.shape[0], up.shape[1]
    moves = [(matrix, k) for matrix in range(2) for k in range(1, T)]

    def columns(matrix, target):
        return spares[matrix].at[:, pl.ds(pl.multiple_of(target * wide, wide), wide)]

    def place(matrix, section, shard):
        start = pl.multiple_of((section * T + shard) * piece, piece)
        return chosen[matrix].at[pl.ds(start, piece), :]

    def spread(matrix, k, landed):
        target = lax.rem(t + k, T)
        dst = place(matrix, s, t) if landed else staged.at[matrix, k]
        sem = piece_recv.at[matrix, s * T + t] if landed else spread_recv.at[matrix, k]
        return pltpu.make_async_remote_copy(
            columns(matrix, target), dst, spread_send.at[matrix, k], sem,
            device_id=(s, target, d), device_id_type=MESH,
        )

    def forward(matrix, k):
        source = lax.rem(t + T - k, T)
        src = staged.at[matrix, k] if k else columns(matrix, t)
        return pltpu.make_async_remote_copy(
            src, place(matrix, s, source), piece_send.at[matrix, k], piece_recv.at[matrix, s * T + source],
            device_id=(failed, t, d), device_id_type=MESH,
        )

    def own_piece(matrix):
        return pltpu.make_async_copy(
            columns(matrix, t), place(matrix, s, t), piece_recv.at[matrix, s * T + t]
        )

    def relay_piece(p):
        matrix, k = moves[p]
        spread(matrix, k, False).wait_recv()
        forward(matrix, k).start()

    @pl.when(is_failed)
    def _():
        for matrix in range(2):
            own_piece(matrix).start()
            for k in range(1, T):
                spread(matrix, k, True).start()

    @pl.when(jnp.logical_not(is_failed))
    def _():
        up_copy.start()
        down_copy.start()
        for matrix in range(2):
            forward(matrix, 0).start()
            for k in range(1, T):
                spread(matrix, k, False).start()

    def weights_ready(matrix):
        @pl.when(is_failed)
        def _():
            def one(i, _):
                section, shard = i // T, lax.rem(i, T)
                pltpu.make_async_copy(
                    columns(matrix, t), place(matrix, section, shard), piece_recv.at[matrix, i]
                ).wait()
                return 0

            lax.fori_loop(0, S * T, one, 0)

        @pl.when(jnp.logical_not(is_failed))
        def _():
            (up_copy, down_copy)[matrix].wait()

    owner = t // (T // R)

    def entering(block, target, how):
        slot = lax.rem(t, T // R) * R + block
        src = inputs_ref.at[pl.ds(0, chunks * group), :, pl.ds(block * width, width)]
        dst = xbuf.at[:, slot, pl.ds(pl.multiple_of(d * tok, tok), tok), :]
        if how == "local":
            return pltpu.make_async_copy(src, dst, start_recv.at[slot, d])
        return pltpu.make_async_remote_copy(
            src, dst, start_send.at[block, target], start_recv.at[slot, d],
            device_id=(s, target, owner), device_id_type=MESH,
        )

    def entering_wait(slot, replica):
        src = inputs_ref.at[pl.ds(0, chunks * group), :, pl.ds(0, width)]
        dst = xbuf.at[:, slot, pl.ds(replica * tok, tok), :]
        pltpu.make_async_copy(src, dst, start_recv.at[slot, replica]).wait()

    @pl.when(first)
    def _():
        for target in range(T):
            for block in range(R):
                mine = (target == t) & (owner == d)

                @pl.when(mine)
                def _():
                    entering(block, target, "local").start()

                @pl.when(jnp.logical_not(mine))
                def _():
                    entering(block, target, "remote").start()

        for slot in range(T):
            for replica in range(R):
                entering_wait(slot, replica)

    def pass_on(c, k):
        target = lax.rem(t + k, T)
        return pltpu.make_async_remote_copy(
            done_buf.at[c], xbuf.at[c, t], x_send.at[c, k], x_recv.at[c, t],
            device_id=(s + 1, target, d), device_id_type=MESH,
        )

    def part_copy(c):
        return pltpu.make_async_remote_copy(
            part_out.at[c], part_in.at[c], part_send.at[c], part_recv.at[c],
            device_id=(s, t, 1 - d), device_id_type=MESH,
        )

    def square_copy(c):
        return pltpu.make_async_remote_copy(
            square_out.at[c], square_in.at[c], square_send.at[c], square_recv.at[c],
            device_id=(s, t, 1 - d), device_id_type=MESH,
        )

    def down_copy_to(c, k):
        target = lax.rem(t + k, T)
        return pltpu.make_async_remote_copy(
            down_out.at[c, k], down_in.at[c, k], down_send.at[c, k], down_recv.at[c, k],
            device_id=(s, target, d), device_id_type=MESH,
        )

    feature_block = d * T + t
    fin_shard, fin_half = feature_block // R, lax.rem(feature_block, R)

    def final_copy(c, g, replica, how):
        batch = c * group + g
        section, slot = batch // per_section, lax.rem(batch, per_section)
        src = done_buf.at[c, pl.ds((g * R + replica) * tok, tok), :]
        dst = fin.at[slot, fin_half]
        sem = fin_recv.at[slot, fin_half]
        if how == "local":
            return section, pltpu.make_async_copy(src, dst, sem)
        return section, pltpu.make_async_remote_copy(
            src, dst, fin_send.at[batch, replica], sem,
            device_id=(section, fin_shard, replica), device_id_type=MESH,
        )

    def is_self(section, replica):
        return (section == s) & (fin_shard == t) & (replica == d)

    def stage_a(c):
        @pl.when(jnp.logical_not(first))
        def _():
            for slot in range(T):
                pltpu.make_async_copy(done_buf.at[c], xbuf.at[c, slot], x_recv.at[c, slot]).wait()

        total = jnp.zeros((rows, 1), jnp.float32)
        pieces = []
        for slot in range(T):
            values = xbuf[c, slot].astype(jnp.float32)
            total = total + jnp.sum(values * values, axis=1, keepdims=True)
            pieces.append((values * gain_ref[:, pl.ds(slot * width, width)]).astype(jnp.bfloat16))
        square_out[c] = jnp.broadcast_to(total, square_out.shape[1:])
        square_copy(c).start()
        scaled = jnp.concatenate(pieces, axis=1)
        part_out[c] = jnp.dot(scaled, up[...], preferred_element_type=jnp.float32).astype(jnp.bfloat16)
        part_copy(c).start()

    def stage_b(c):
        square_copy(c).wait_recv()
        part_copy(c).wait_recv()
        mean_square = (square_out[c][:, :1] + square_in[c][:, :1]) * (1.0 / model)
        pre = part_out[c].astype(jnp.float32) + part_in[c].astype(jnp.float32)
        pre = pre * lax.rsqrt(mean_square + 1e-05)
        hidden = (pre / (1.0 + jnp.exp(-pre))).astype(jnp.bfloat16)

        def block_sum(i, _):
            k = lax.rem(i + 1, T)
            target = lax.rem(t + k, T)
            block = down[pl.ds(pl.multiple_of(target * width, width), width), :]
            down_out[c, k] = lax.dot_general(
                hidden, block, (((1,), (1,)), ((), ())), preferred_element_type=jnp.float32
            ).astype(jnp.bfloat16)

            @pl.when(k > 0)
            def _():
                down_copy_to(c, k).start()

            return 0

        lax.fori_loop(0, T, block_sum, 0)

    def stage_c(c):
        acc = xbuf[c, t].astype(jnp.float32) + down_out[c, 0].astype(jnp.float32)
        for k in range(1, T):
            down_copy_to(c, k).wait_recv()
            acc = acc + down_in[c, k].astype(jnp.float32)
        done_buf[c] = acc.astype(jnp.bfloat16)

        @pl.when(jnp.logical_not(last))
        def _():
            for k in range(T):
                pass_on(c, k).start()

        @pl.when(last)
        def _():
            for g in range(group):
                for replica in range(R):
                    section, local = final_copy(c, g, replica, "local")
                    _, remote = final_copy(c, g, replica, "remote")
                    mine = is_self(section, replica)

                    @pl.when(mine)
                    def _():
                        local.start()

                    @pl.when(jnp.logical_not(mine))
                    def _():
                        remote.start()

    early = 2 * s
    for p in range(len(moves)):

        @pl.when((s > failed) | ((s < failed) & (p < early)))
        def _():
            relay_piece(p)

    def step(i, _):
        @pl.when(i == 0)
        def _():
            weights_ready(0)

        @pl.when(i == 1)
        def _():
            weights_ready(1)

        @pl.when(i < chunks)
        def _():
            stage_a(i)

        @pl.when((i >= 1) & (i < chunks + 1))
        def _():
            stage_b(i - 1)

        @pl.when(i >= 2)
        def _():
            stage_c(i - 2)

        for p in range(len(moves)):

            @pl.when((s < failed) & (i + early == p))
            def _():
                relay_piece(p)

        return 0

    lax.fori_loop(0, chunks + 2, step, 0)
    for p in range(len(moves)):

        @pl.when((s < failed) & (p >= early + chunks + 2))
        def _():
            relay_piece(p)

    for slot in range(per_section):
        runs = s * per_section + slot < chunks * group

        @pl.when(runs)
        def _():
            for half in range(R):
                pltpu.make_async_copy(
                    done_buf.at[0, pl.ds(0, tok), :], fin.at[slot, half], fin_recv.at[slot, half]
                ).wait()
                finals_ref[slot, :, pl.ds(half * width, width)] = fin[slot, half]

        @pl.when(jnp.logical_not(runs))
        def _():
            finals_ref[slot] = jnp.zeros(finals_ref.shape[1:], finals_ref.dtype)

    @pl.when(is_failed)
    def _():
        for matrix, k in moves:
            spread(matrix, k, True).wait_send()

    @pl.when(jnp.logical_not(is_failed))
    def _():
        for matrix in range(2):
            forward(matrix, 0).wait_send()
        for matrix, k in moves:
            spread(matrix, k, False).wait_send()
            forward(matrix, k).wait_send()

    @pl.when(first)
    def _():
        for target in range(T):
            for block in range(R):

                @pl.when(jnp.logical_not((target == t) & (owner == d)))
                def _():
                    entering(block, target, "remote").wait_send()

    def drain(c, _):
        square_copy(c).wait_send()
        part_copy(c).wait_send()
        for k in range(1, T):
            down_copy_to(c, k).wait_send()

        @pl.when(jnp.logical_not(last))
        def _():
            for k in range(T):
                pass_on(c, k).wait_send()

        @pl.when(last)
        def _():
            for g in range(group):
                for replica in range(R):
                    section, remote = final_copy(c, g, replica, "remote")

                    @pl.when(jnp.logical_not(is_self(section, replica)))
                    def _():
                        remote.wait_send()

        return 0

    lax.fori_loop(0, chunks, drain, 0)


def relay(entering, gain, up, down, spare_up, spare_down, S, T, R, chunks, failed):
    batches, tok, share = entering.shape
    group = 1
    rows = group * R * tok
    width = share // R
    wide = up.shape[1]
    bf16, f32 = jnp.bfloat16, jnp.float32
    dma = pltpu.SemaphoreType.DMA
    vmem = pl.BlockSpec(memory_space=pltpu.VMEM)
    hbm = pl.BlockSpec(memory_space=pl.ANY)
    return pl.pallas_call(
        functools.partial(relay_kernel, (S, T, R, chunks, group, tok), failed),
        out_shape=jax.ShapeDtypeStruct((batches // S, tok, share), bf16),
        in_specs=[vmem, vmem, hbm, hbm, hbm, hbm],
        out_specs=vmem,
        scratch_shapes=[
            pltpu.VMEM(up.shape, bf16),
            pltpu.VMEM(down.shape, bf16),
            pltpu.VMEM((chunks, T, rows, width), bf16),
            pltpu.VMEM((chunks, rows, wide), bf16),
            pltpu.VMEM((chunks, rows, wide), bf16),
            pltpu.VMEM((chunks, rows, 128), f32),
            pltpu.VMEM((chunks, rows, 128), f32),
            pltpu.VMEM((chunks, T, rows, width), bf16),
            pltpu.VMEM((chunks, T, rows, width), bf16),
            pltpu.VMEM((chunks, rows, width), bf16),
            pltpu.VMEM((batches // S, R, tok, width), bf16),
            pltpu.VMEM((2, T, spare_up.shape[0], wide), bf16),
            dma((2,)),
            dma((2, T)),
            dma((2, T)),
            dma((2, T)),
            dma((2, S * T)),
            dma((R, T)),
            dma((T, R)),
            dma((chunks, T)),
            dma((chunks, T)),
            dma((chunks,)),
            dma((chunks,)),
            dma((chunks,)),
            dma((chunks,)),
            dma((chunks, T)),
            dma((chunks, T)),
            dma((batches, R)),
            dma((batches // S, R)),
        ],
        compiler_params=pltpu.CompilerParams(has_side_effects=True, vmem_limit_bytes=60 * 1024 * 1024),
    )(entering, gain, up, down, spare_up, spare_down)


TIMES = dict(A=0, B=2, C=4, next=6, FA=0, FB=3, FC=5, FD=7, FE=9, FG=10, after=12, period=4)


def shared_kernel(
    sizes,
    failed,
    inputs_ref,
    gain_ref,
    up_hbm,
    down_hbm,
    spare_up,
    spare_down,
    finals_ref,
    up,
    down,
    xbuf,
    part_out,
    part_in,
    down_out,
    down_in,
    done_buf,
    fin,
    f_up,
    f_down,
    f_gain,
    f_x,
    f_part,
    f_cross_in,
    f_line_out,
    f_line_in,
    f_hid,
    f_own,
    f_out,
    f_in,
    f_done,
    weight_sem,
    swap_send,
    swap_recv,
    gain_send,
    gain_recv,
    start_send,
    x_send,
    x_recv,
    part_send,
    part_recv,
    down_send,
    down_recv,
    fin_send,
    fin_recv,
    fx_recv,
    cross_send,
    cross_recv,
    line_send,
    line_recv,
    hid_line_send,
    hid_line_recv,
    hid_cross_send,
    hid_cross_recv,
    pair_send,
    pair_recv,
):
    S, T, R, chunks, tok = sizes
    s, t, d = lax.axis_index("section"), lax.axis_index("tensor"), lax.axis_index("dp")
    rows = R * tok
    width = xbuf.shape[-1]
    model = width * T * R
    wide = up.shape[1]
    piece = spare_up.shape[0]
    half = f_up.shape[2]
    groups = S // 2 * R
    quarter = half // groups
    strip = rows // T
    per_section = finals_ref.shape[0]
    bf16, f32 = jnp.bfloat16, jnp.float32
    core, chip = lax.rem(s, 2), s // 2
    partner = s + 1 - 2 * core
    mine = chip * R + d
    is_failed, not_failed = s == failed, s != failed
    last_failed, first_failed = failed == S - 1, failed == 0

    up_copy = pltpu.make_async_copy(up_hbm, up, weight_sem.at[0])
    down_copy = pltpu.make_async_copy(down_hbm, down, weight_sem.at[1])

    def remote(src, dst, send, recv, where):
        return pltpu.make_async_remote_copy(src, dst, send, recv, device_id=where, device_id_type=MESH)

    def route(src, dst, send, recv, where):
        return where, lambda: pltpu.make_async_copy(src, dst, recv), lambda: remote(src, dst, send, recv, where)

    def is_self(where):
        return (where[0] == s) & (where[1] == t) & (where[2] == d)

    def go(routed):
        where, local, far = routed
        here = is_self(where)

        @pl.when(here)
        def _():
            local().start()

        @pl.when(jnp.logical_not(here))
        def _():
            far().start()

    def sent(routed):
        where, _, far = routed

        @pl.when(jnp.logical_not(is_self(where)))
        def _():
            far().wait_send()

    def landed(ref, sem):
        pltpu.make_async_copy(ref, ref, sem).wait()

    spares, pair_weights = (spare_up, spare_down), (f_up, f_down)

    def swap_src(matrix, side):
        return spares[matrix].at[:, pl.ds(pl.multiple_of(side * half, half), half)]

    def swap_own(matrix):
        return pltpu.make_async_copy(swap_src(matrix, core), pair_weights[matrix].at[core], weight_sem.at[2 + matrix])

    def swap_far(matrix):
        return remote(
            swap_src(matrix, 1 - core), pair_weights[matrix].at[core],
            swap_send.at[matrix], swap_recv.at[matrix], (partner, t, d),
        )

    def swap_ready(matrix):
        swap_own(matrix).wait()
        swap_far(matrix).wait_recv()

    def gain_route(target, side):
        start = d * (T * width) + (target // 2 * 2 + side) * width + t * piece
        src = gain_ref.at[:, pl.ds(pl.multiple_of(start, piece), piece)]
        return route(src, f_gain.at[side], gain_send.at[target, side], gain_recv.at[0], (target, t, d))

    owner = t // (T // R)

    def entering(c, target, block):
        slot = lax.rem(t, T // R) * R + block
        src = inputs_ref.at[c, :, pl.ds(block * width, width)]
        dst = xbuf.at[c, slot, pl.ds(pl.multiple_of(d * tok, tok), tok), :]
        return route(src, dst, start_send.at[c, target, block], x_recv.at[c], (s, target, owner))

    def entering_spare(c, target, side):
        src = inputs_ref.at[c, :, pl.ds(pl.multiple_of(side * width + target * piece, piece), piece)]
        dst = f_x.at[c, pl.ds(pl.multiple_of(d * tok, tok), tok), pl.ds(side * piece, piece)]
        return route(src, dst, start_send.at[c, target, side], fx_recv.at[c], (s, target, owner))

    enters = (chip == lax.rem(t, T // R)) if first_failed else (s == 0)
    entry = entering_spare if first_failed else entering

    def pass_on(c, target):
        return route(done_buf.at[c], xbuf.at[c, t], x_send.at[c, target], x_recv.at[c], (s + 1, target, d))

    def pass_spare(c, target, side):
        src = done_buf.at[c, :, pl.ds(pl.multiple_of(target * piece, piece), piece)]
        dst = f_x.at[c, :, pl.ds(pl.multiple_of(lax.rem(t, 2) * piece, piece), piece)]
        return route(src, dst, x_send.at[c, target * 2 + side], fx_recv.at[c], (t // 2 * 2 + side, target, d))

    def leave_spare(c, target):
        dst = xbuf.at[c, s, :, pl.ds(pl.multiple_of(t * piece, piece), piece)]
        return route(f_done.at[c], dst, hid_cross_send.at[c, T * groups + target], x_recv.at[c], (failed + 1, target, d))

    def final_normal(c, replica):
        block = d * T + t
        dst = fin.at[lax.rem(c, per_section), :, pl.ds(pl.multiple_of(lax.rem(block, R) * width, width), width)]
        return route(
            done_buf.at[c, pl.ds(replica * tok, tok), :], dst, fin_send.at[c, replica],
            fin_recv.at[lax.rem(c, per_section)], (c // per_section, block // R, replica),
        )

    def final_spare(c, replica):
        block = d * T + s
        start = pl.multiple_of(lax.rem(block, R) * width + t * piece, piece)
        return route(
            f_done.at[c, pl.ds(replica * tok, tok), :], fin.at[lax.rem(c, per_section), :, pl.ds(start, piece)],
            fin_send.at[c, replica], fin_recv.at[lax.rem(c, per_section)], (c // per_section, block // R, replica),
        )

    def part_copy(c):
        return remote(part_out.at[c], part_in.at[c], part_send.at[c], part_recv.at[c], (s, t, 1 - d))

    def down_copy_to(c, target):
        slot = lax.rem(target + T - t, T) - 1
        return remote(down_out.at[c, target], down_in.at[c, slot], down_send.at[c, target], down_recv.at[c], (s, target, d))

    def square_block(total):
        coarse = total.astype(bf16).astype(f32)
        lane = lax.broadcasted_iota(jnp.int32, (total.shape[0], 128), 1)
        return jnp.where(lane < 64, coarse, total - coarse).astype(bf16)

    def square_of(block):
        return block[:, 0:1] + block[:, 64:65]

    def stage_a(c):
        landed(xbuf.at[c], x_recv.at[c])
        total = jnp.zeros((rows, 1), f32)
        pieces = []
        for slot in range(T):
            values = xbuf[c, slot].astype(f32)
            total = total + jnp.sum(values * values, axis=1, keepdims=True)
            gain = gain_ref[:, pl.ds(slot * width, width)]
            for other in range(1, R):
                gain = jnp.where(d == other, gain_ref[:, pl.ds((other * T + slot) * width, width)], gain)
            pieces.append((values * gain).astype(bf16))
        part_out[c, :, pl.ds(wide, 128)] = square_block(total)
        scaled = jnp.concatenate(pieces, axis=1)
        part_out[c, :, pl.ds(0, wide)] = jnp.dot(scaled, up[...], preferred_element_type=f32).astype(bf16)
        part_copy(c).start()

    def stage_b(c):
        part_copy(c).wait_recv()
        both = part_out[c].astype(f32) + part_in[c].astype(f32)
        mean_square = square_of(both[:, wide:]) * (1.0 / model)
        pre = both[:, :wide] * lax.rsqrt(mean_square + 1e-05)
        hidden = (pre / (1.0 + jnp.exp(-pre))).astype(bf16)

        def block_sum(i, _):
            target = jnp.where(t < T // 2, T - 1 - i, i)
            block = down[pl.ds(pl.multiple_of(target * width, width), width), :]
            down_out[c, target] = lax.dot_general(
                hidden, block, (((1,), (1,)), ((), ())), preferred_element_type=f32
            ).astype(bf16)

            @pl.when(target != t)
            def _():
                down_copy_to(c, target).start()

            return 0

        lax.fori_loop(0, T, block_sum, 0)

    def stage_c(c):
        landed(down_in.at[c], down_recv.at[c])
        acc = xbuf[c, t].astype(f32) + down_out[c, t].astype(f32)
        for k in range(T - 1):
            acc = acc + down_in[c, k].astype(f32)
        done_buf[c] = acc.astype(bf16)
        each_next(c, go)

    def each_next(c, act):
        if failed > 0:

            @pl.when(s == failed - 1)
            def _():
                for target in range(T):
                    for side in range(2):
                        act(pass_spare(c, target, side))

        @pl.when((s != failed - 1) & (s < S - 1))
        def _():
            for target in range(T):
                act(pass_on(c, target))

        if not last_failed:

            @pl.when(s == S - 1)
            def _():
                for replica in range(R):
                    act(final_normal(c, replica))

    def each_after(c, act):
        if last_failed:
            for replica in range(R):
                act(final_spare(c, replica))
        else:
            for target in range(T):
                act(leave_spare(c, target))

    def other_group(k):
        return lax.rem(mine + k, groups)

    def group_device(g, line):
        return (g // R * 2 + core, line, lax.rem(g, R))

    def cross_copy(c, k):
        g = other_group(k)
        return remote(
            f_part.at[c, g], f_cross_in.at[c, k - 1], cross_send.at[c, k], cross_recv.at[c], group_device(g, t)
        )

    def line_copy(c, k):
        target = lax.rem(t + k, T)
        src = f_line_out.at[c, pl.ds(pl.multiple_of(target * strip, strip), strip), :]
        return remote(src, f_line_in.at[c, k - 1], line_send.at[c, k], line_recv.at[c], (s, target, d))

    def hid_at(c, line):
        return f_hid.at[c, mine, pl.ds(pl.multiple_of(line * strip, strip), strip), :]

    def hid_line_copy(c, k):
        target = lax.rem(t + k, T)
        return remote(hid_at(c, t), hid_at(c, t), hid_line_send.at[c, k], hid_line_recv.at[c, t], (s, target, d))

    def hid_cross_copy(c, k, line):
        where = group_device(other_group(k), t)
        return remote(
            hid_at(c, line), hid_at(c, line), hid_cross_send.at[c, k * T + line], hid_cross_recv.at[c, mine], where
        )

    def pair_copy(c):
        return remote(f_out.at[c], f_in.at[c], pair_send.at[c], pair_recv.at[c], (partner, t, d))

    def own_columns(block):
        return jnp.where(core == 0, block[:, :piece], block[:, piece:])

    def spare_a(c):
        landed(f_x.at[c], fx_recv.at[c])
        values = f_x[c].astype(f32)
        squares = square_block(jnp.sum(values * values, axis=1, keepdims=True))
        gain = jnp.concatenate([f_gain[0], f_gain[1]], axis=1)
        scaled = (values * gain).astype(bf16)
        weights = jnp.concatenate([f_up[0], f_up[1]], axis=0)
        product = jnp.dot(scaled, weights, preferred_element_type=f32).astype(bf16)
        for g in range(groups):
            f_part[c, g, :, pl.ds(0, quarter)] = product[:, g * quarter : (g + 1) * quarter]
            f_part[c, g, :, pl.ds(quarter, 128)] = squares
        for k in range(1, groups):
            cross_copy(c, k).start()

    def spare_b(c):
        landed(f_cross_in.at[c], cross_recv.at[c])
        total = f_part[c, mine].astype(f32)
        for k in range(groups - 1):
            total = total + f_cross_in[c, k].astype(f32)
        f_line_out[c, :, pl.ds(0, quarter)] = total[:, :quarter].astype(bf16)
        f_line_out[c, :, pl.ds(quarter, 128)] = square_block(square_of(total[:, quarter:]))
        for k in range(1, T):
            line_copy(c, k).start()

    def spare_c(c):
        landed(f_line_in.at[c], line_recv.at[c])
        at = pl.ds(pl.multiple_of(t * strip, strip), strip)
        total = f_line_out[c, at, :].astype(f32)
        for k in range(T - 1):
            total = total + f_line_in[c, k].astype(f32)
        mean_square = square_of(total[:, quarter:]) * (1.0 / model)
        pre = total[:, :quarter] * lax.rsqrt(mean_square + 1e-05)
        f_hid[c, mine, at, :] = (pre / (1.0 + jnp.exp(-pre))).astype(bf16)
        for k in range(1, T):
            hid_line_copy(c, k).start()
        for k in range(1, groups):
            hid_cross_copy(c, k, t).start()

    def spare_d(c):
        for j in range(1, T):
            line = lax.rem(t + j, T)
            landed(hid_at(c, line), hid_line_recv.at[c, line])
            for k in range(1, groups):
                hid_cross_copy(c, k, line).start()

    def spare_e(c):
        for k in range(1, groups):
            g = other_group(k)
            landed(f_hid.at[c, g], hid_cross_recv.at[c, g])
        hidden = jnp.concatenate([f_hid[c, g] for g in range(groups)], axis=1)
        weights = jnp.concatenate([f_down[0], f_down[1]], axis=0)
        result = lax.dot_general(hidden, weights, (((1,), (1,)), ((), ())), preferred_element_type=f32)
        f_out[c] = jnp.where(core == 0, result[:, piece:], result[:, :piece]).astype(bf16)
        pair_copy(c).start()
        f_own[c] = own_columns(result)

    def spare_g(c):
        pair_copy(c).wait_recv()
        acc = own_columns(f_x[c].astype(f32)) + f_own[c] + f_in[c].astype(f32)
        f_done[c] = acc.astype(bf16)
        each_after(c, go)

    @pl.when(enters)
    def _():
        def one(c, _):
            for target in range(T):
                for part in range(R):
                    go(entry(c, target, part))
            return 0

        lax.fori_loop(0, chunks, one, 0)

    @pl.when(not_failed)
    def _():
        up_copy.start()
        down_copy.start()

    for matrix in range(2):
        swap_own(matrix).start()
        swap_far(matrix).start()

    @pl.when(is_failed)
    def _():
        for target in range(S):
            for side in range(2):
                go(gain_route(target, side))

    period = TIMES["period"]
    begin = jnp.where(s > failed, (s - 1) * TIMES["next"] + TIMES["after"], s * TIMES["next"])
    spare_begin = failed * TIMES["next"]
    steps = (S - 1) * TIMES["next"] + TIMES["after"] + period * (chunks - 1)

    def step(i, _):
        def at(offset, allowed, stage):
            since = i - offset
            due = (since >= 0) & (since < chunks * period) & (lax.rem(since + period * steps, period) == 0)

            @pl.when(due if allowed is None else due & allowed)
            def _():
                stage(since // period)

        def first_time(c, ready):
            @pl.when(c == 0)
            def _():
                ready()

        def a(c):
            first_time(c, up_copy.wait)
            stage_a(c)

        def b(c):
            first_time(c, down_copy.wait)
            stage_b(c)

        def fa(c):
            def ready():
                swap_ready(0)
                landed(f_gain, gain_recv.at[0])

            first_time(c, ready)
            spare_a(c)

        def fe(c):
            first_time(c, lambda: swap_ready(1))
            spare_e(c)

        at(spare_begin + TIMES["FG"], None, spare_g)
        at(spare_begin + TIMES["FE"], None, fe)
        at(spare_begin + TIMES["FD"], None, spare_d)
        at(spare_begin + TIMES["FC"], None, spare_c)
        at(begin + TIMES["C"], not_failed, stage_c)
        at(begin + TIMES["B"], not_failed, b)
        at(spare_begin + TIMES["FB"], None, spare_b)
        at(spare_begin + TIMES["FA"], None, fa)
        at(begin + TIMES["A"], not_failed, a)
        return 0

    lax.fori_loop(0, steps, step, 0)

    for slot in range(per_section):
        runs = s * per_section + slot < chunks

        @pl.when(runs)
        def _():
            landed(fin.at[slot], fin_recv.at[slot])
            finals_ref[slot] = fin[slot]

        @pl.when(jnp.logical_not(runs))
        def _():
            finals_ref[slot] = jnp.zeros(finals_ref.shape[1:], finals_ref.dtype)

    for matrix in range(2):
        swap_far(matrix).wait_send()

    @pl.when(is_failed)
    def _():
        for target in range(S):
            for side in range(2):
                sent(gain_route(target, side))

    def drain(c, _):
        @pl.when(enters)
        def _():
            for target in range(T):
                for part in range(R):
                    sent(entry(c, target, part))

        @pl.when(not_failed)
        def _():
            part_copy(c).wait_send()

            def one(target, _):
                @pl.when(target != t)
                def _():
                    down_copy_to(c, target).wait_send()

                return 0

            lax.fori_loop(0, T, one, 0)
            each_next(c, sent)

        for k in range(1, groups):
            cross_copy(c, k).wait_send()

            def line_sent(line, _):
                hid_cross_copy(c, k, line).wait_send()
                return 0

            lax.fori_loop(0, T, line_sent, 0)
        for k in range(1, T):
            line_copy(c, k).wait_send()
            hid_line_copy(c, k).wait_send()
        pair_copy(c).wait_send()
        each_after(c, sent)
        return 0

    lax.fori_loop(0, chunks, drain, 0)


def shared(entering, gain, up, down, spare_up, spare_down, S, T, R, chunks, failed):
    batches, tok, share = entering.shape
    rows = R * tok
    width = share // R
    wide = up.shape[1]
    piece = spare_up.shape[0]
    half = spare_up.shape[1] // 2
    groups = S // 2 * R
    quarter = half // groups
    strip = rows // T
    bf16, f32 = jnp.bfloat16, jnp.float32
    dma = pltpu.SemaphoreType.DMA
    vmem = pl.BlockSpec(memory_space=pltpu.VMEM)
    hbm = pl.BlockSpec(memory_space=pl.ANY)
    per_section = batches // S
    return pl.pallas_call(
        functools.partial(shared_kernel, (S, T, R, chunks, tok), failed),
        out_shape=jax.ShapeDtypeStruct((per_section, tok, share), bf16),
        in_specs=[vmem, vmem, hbm, hbm, hbm, hbm],
        out_specs=vmem,
        scratch_shapes=[
            pltpu.VMEM(up.shape, bf16),
            pltpu.VMEM(down.shape, bf16),
            pltpu.VMEM((chunks, T, rows, width), bf16),
            pltpu.VMEM((chunks, rows, wide + 128), bf16),
            pltpu.VMEM((chunks, rows, wide + 128), bf16),
            pltpu.VMEM((chunks, T, rows, width), bf16),
            pltpu.VMEM((chunks, T - 1, rows, width), bf16),
            pltpu.VMEM((chunks, rows, width), bf16),
            pltpu.VMEM((per_section, tok, share), bf16),
            pltpu.VMEM((2, piece, half), bf16),
            pltpu.VMEM((2, piece, half), bf16),
            pltpu.VMEM((2, 1, piece), f32),
            pltpu.VMEM((chunks, rows, 2 * piece), bf16),
            pltpu.VMEM((chunks, groups, rows, quarter + 128), bf16),
            pltpu.VMEM((chunks, groups - 1, rows, quarter + 128), bf16),
            pltpu.VMEM((chunks, rows, quarter + 128), bf16),
            pltpu.VMEM((chunks, T - 1, strip, quarter + 128), bf16),
            pltpu.VMEM((chunks, groups, rows, quarter), bf16),
            pltpu.VMEM((chunks, rows, piece), f32),
            pltpu.VMEM((chunks, rows, piece), bf16),
            pltpu.VMEM((chunks, rows, piece), bf16),
            pltpu.VMEM((chunks, rows, piece), bf16),
            dma((4,)),
            dma((2,)),
            dma((2,)),
            dma((S, 2)),
            dma((1,)),
            dma((chunks, T, R)),
            dma((chunks, 2 * T)),
            dma((chunks,)),
            dma((chunks,)),
            dma((chunks,)),
            dma((chunks, T)),
            dma((chunks,)),
            dma((chunks, R)),
            dma((per_section,)),
            dma((chunks,)),
            dma((chunks, groups)),
            dma((chunks,)),
            dma((chunks, T)),
            dma((chunks,)),
            dma((chunks, T)),
            dma((chunks, T)),
            dma((chunks, T * groups + T)),
            dma((chunks, groups)),
            dma((chunks,)),
            dma((chunks,)),
        ],
        compiler_params=pltpu.CompilerParams(has_side_effects=True, vmem_limit_bytes=60 * 1024 * 1024),
    )(entering, gain, up, down, spare_up, spare_down)


def spreads(S, T, R, tok, share, piece, columns):
    width, rows = share // R, R * tok
    groups = S // 2 * R
    fits = S == T and S % 2 == 0 and T % 2 == 0 and R == 2 and T // R * R == T and T // R == S // 2
    return fits and width == T * piece and piece % 128 == 0 and columns % (256 * groups) == 0 and rows % (16 * T) == 0


def body(
    section_up,
    section_down,
    backup_up,
    backup_down,
    norm_gain,
    micro_batches,
    failed_section,
    live_batches,
):
    S, T, R = lax.axis_size("section"), lax.axis_size("tensor"), lax.axis_size("dp")
    batch_count, tok, share = micro_batches.shape
    live_count = batch_count // 2 + live_batches[0] % (batch_count - batch_count // 2 + 1)
    spare_up = backup_up.reshape(backup_up.shape[3:])
    spare_down = backup_down.reshape(backup_down.shape[3:])
    least = batch_count // 2
    stride = -(-(batch_count - least + 1) // 3)
    counts = list(range(batch_count, least - 1, -stride))
    chosen = (batch_count - live_count) // stride
    entering = micro_batches
    if stride > 1:
        alive = lax.broadcasted_iota(jnp.int32, (batch_count, 1, 1), 0) < live_count
        entering = jnp.where(alive, micro_batches, jnp.zeros_like(micro_batches))
    gain, call = norm_gain, shared
    if not spreads(S, T, R, tok, share, *spare_up.shape):
        depth = section_up.shape[1]
        gain = lax.dynamic_slice_in_dim(norm_gain, lax.axis_index("dp") * depth, depth, 1)
        call = relay
    operands = (entering, gain, section_up[0], section_down[0], spare_up, spare_down)

    def variant(failed, count):
        return lambda *arrays: call(*arrays, S, T, R, count, failed)

    variants = [variant(f, count) for count in counts for f in range(S)]
    return lax.switch(chosen * S + failed_section[0] % S, variants, *operands)


def solution(mesh):
    placed = (
        P("section", "dp", "tensor"),
        P("section", "dp", "tensor"),
        P("dp", "section", "tensor", None, None),
        P("dp", "section", "tensor", None, None),
        P("section", None),
        P(None, "dp", "tensor"),
        P(),
        P(),
    )
    return jax.shard_map(
        body, mesh=mesh, in_specs=placed, out_specs=P("section", "dp", "tensor"), check_vma=False
    )
```

```python
import functools

import jax
import jax.numpy as jnp
from jax import lax
from jax.experimental import pallas as pl
from jax.experimental.pallas import tpu as pltpu
from jax.sharding import PartitionSpec as P

MESH = pl.DeviceIdType.MESH


def relay_kernel(
    sizes,
    failed,
    inputs_ref,
    gain_ref,
    up_hbm,
    down_hbm,
    spare_up,
    spare_down,
    finals_ref,
    up,
    down,
    xbuf,
    part_out,
    part_in,
    square_out,
    square_in,
    down_out,
    down_in,
    done_buf,
    fin,
    staged,
    weight_sem,
    spread_send,
    spread_recv,
    piece_send,
    piece_recv,
    start_send,
    start_recv,
    x_send,
    x_recv,
    part_send,
    part_recv,
    square_send,
    square_recv,
    down_send,
    down_recv,
    fin_send,
    fin_recv,
):
    S, T, R, chunks, group, tok = sizes
    s, t, d = lax.axis_index("section"), lax.axis_index("tensor"), lax.axis_index("dp")
    rows = group * R * tok
    width = xbuf.shape[-1]
    model = width * T * R
    first, last = s == 0, s == S - 1
    per_section = finals_ref.shape[0]

    is_failed = s == failed
    up_copy = pltpu.make_async_copy(up_hbm, up, weight_sem.at[0])
    down_copy = pltpu.make_async_copy(down_hbm, down, weight_sem.at[1])
    spares, chosen = (spare_up, spare_down), (up, down)
    piece, wide = spare_up.shape[0], up.shape[1]
    moves = [(matrix, k) for matrix in range(2) for k in range(1, T)]

    def columns(matrix, target):
        return spares[matrix].at[:, pl.ds(pl.multiple_of(target * wide, wide), wide)]

    def place(matrix, section, shard):
        start = pl.multiple_of((section * T + shard) * piece, piece)
        return chosen[matrix].at[pl.ds(start, piece), :]

    def spread(matrix, k, landed):
        target = lax.rem(t + k, T)
        dst = place(matrix, s, t) if landed else staged.at[matrix, k]
        sem = piece_recv.at[matrix, s * T + t] if landed else spread_recv.at[matrix, k]
        return pltpu.make_async_remote_copy(
            columns(matrix, target), dst, spread_send.at[matrix, k], sem,
            device_id=(s, target, d), device_id_type=MESH,
        )

    def forward(matrix, k):
        source = lax.rem(t + T - k, T)
        src = staged.at[matrix, k] if k else columns(matrix, t)
        return pltpu.make_async_remote_copy(
            src, place(matrix, s, source), piece_send.at[matrix, k], piece_recv.at[matrix, s * T + source],
            device_id=(failed, t, d), device_id_type=MESH,
        )

    def own_piece(matrix):
        return pltpu.make_async_copy(
            columns(matrix, t), place(matrix, s, t), piece_recv.at[matrix, s * T + t]
        )

    def relay_piece(p):
        matrix, k = moves[p]
        spread(matrix, k, False).wait_recv()
        forward(matrix, k).start()

    @pl.when(is_failed)
    def _():
        for matrix in range(2):
            own_piece(matrix).start()
            for k in range(1, T):
                spread(matrix, k, True).start()

    @pl.when(jnp.logical_not(is_failed))
    def _():
        up_copy.start()
        down_copy.start()
        for matrix in range(2):
            forward(matrix, 0).start()
            for k in range(1, T):
                spread(matrix, k, False).start()

    def weights_ready(matrix):
        @pl.when(is_failed)
        def _():
            def one(i, _):
                section, shard = i // T, lax.rem(i, T)
                pltpu.make_async_copy(
                    columns(matrix, t), place(matrix, section, shard), piece_recv.at[matrix, i]
                ).wait()
                return 0

            lax.fori_loop(0, S * T, one, 0)

        @pl.when(jnp.logical_not(is_failed))
        def _():
            (up_copy, down_copy)[matrix].wait()

    owner = t // (T // R)

    def entering(block, target, how):
        slot = lax.rem(t, T // R) * R + block
        src = inputs_ref.at[pl.ds(0, chunks * group), :, pl.ds(block * width, width)]
        dst = xbuf.at[:, slot, pl.ds(pl.multiple_of(d * tok, tok), tok), :]
        if how == "local":
            return pltpu.make_async_copy(src, dst, start_recv.at[slot, d])
        return pltpu.make_async_remote_copy(
            src, dst, start_send.at[block, target], start_recv.at[slot, d],
            device_id=(s, target, owner), device_id_type=MESH,
        )

    def entering_wait(slot, replica):
        src = inputs_ref.at[pl.ds(0, chunks * group), :, pl.ds(0, width)]
        dst = xbuf.at[:, slot, pl.ds(replica * tok, tok), :]
        pltpu.make_async_copy(src, dst, start_recv.at[slot, replica]).wait()

    @pl.when(first)
    def _():
        for target in range(T):
            for block in range(R):
                mine = (target == t) & (owner == d)

                @pl.when(mine)
                def _():
                    entering(block, target, "local").start()

                @pl.when(jnp.logical_not(mine))
                def _():
                    entering(block, target, "remote").start()

        for slot in range(T):
            for replica in range(R):
                entering_wait(slot, replica)

    def pass_on(c, k):
        target = lax.rem(t + k, T)
        return pltpu.make_async_remote_copy(
            done_buf.at[c], xbuf.at[c, t], x_send.at[c, k], x_recv.at[c, t],
            device_id=(s + 1, target, d), device_id_type=MESH,
        )

    def part_copy(c):
        return pltpu.make_async_remote_copy(
            part_out.at[c], part_in.at[c], part_send.at[c], part_recv.at[c],
            device_id=(s, t, 1 - d), device_id_type=MESH,
        )

    def square_copy(c):
        return pltpu.make_async_remote_copy(
            square_out.at[c], square_in.at[c], square_send.at[c], square_recv.at[c],
            device_id=(s, t, 1 - d), device_id_type=MESH,
        )

    def down_copy_to(c, k):
        target = lax.rem(t + k, T)
        return pltpu.make_async_remote_copy(
            down_out.at[c, k], down_in.at[c, k], down_send.at[c, k], down_recv.at[c, k],
            device_id=(s, target, d), device_id_type=MESH,
        )

    feature_block = d * T + t
    fin_shard, fin_half = feature_block // R, lax.rem(feature_block, R)

    def final_copy(c, g, replica, how):
        batch = c * group + g
        section, slot = batch // per_section, lax.rem(batch, per_section)
        src = done_buf.at[c, pl.ds((g * R + replica) * tok, tok), :]
        dst = fin.at[slot, fin_half]
        sem = fin_recv.at[slot, fin_half]
        if how == "local":
            return section, pltpu.make_async_copy(src, dst, sem)
        return section, pltpu.make_async_remote_copy(
            src, dst, fin_send.at[batch, replica], sem,
            device_id=(section, fin_shard, replica), device_id_type=MESH,
        )

    def is_self(section, replica):
        return (section == s) & (fin_shard == t) & (replica == d)

    def stage_a(c):
        @pl.when(jnp.logical_not(first))
        def _():
            for slot in range(T):
                pltpu.make_async_copy(done_buf.at[c], xbuf.at[c, slot], x_recv.at[c, slot]).wait()

        total = jnp.zeros((rows, 1), jnp.float32)
        pieces = []
        for slot in range(T):
            values = xbuf[c, slot].astype(jnp.float32)
            total = total + jnp.sum(values * values, axis=1, keepdims=True)
            pieces.append((values * gain_ref[:, pl.ds(slot * width, width)]).astype(jnp.bfloat16))
        square_out[c] = jnp.broadcast_to(total, square_out.shape[1:])
        square_copy(c).start()
        scaled = jnp.concatenate(pieces, axis=1)
        part_out[c] = jnp.dot(scaled, up[...], preferred_element_type=jnp.float32).astype(jnp.bfloat16)
        part_copy(c).start()

    def stage_b(c):
        square_copy(c).wait_recv()
        part_copy(c).wait_recv()
        mean_square = (square_out[c][:, :1] + square_in[c][:, :1]) * (1.0 / model)
        pre = part_out[c].astype(jnp.float32) + part_in[c].astype(jnp.float32)
        pre = pre * lax.rsqrt(mean_square + 1e-05)
        hidden = (pre / (1.0 + jnp.exp(-pre))).astype(jnp.bfloat16)

        def block_sum(i, _):
            k = lax.rem(i + 1, T)
            target = lax.rem(t + k, T)
            block = down[pl.ds(pl.multiple_of(target * width, width), width), :]
            down_out[c, k] = lax.dot_general(
                hidden, block, (((1,), (1,)), ((), ())), preferred_element_type=jnp.float32
            ).astype(jnp.bfloat16)

            @pl.when(k > 0)
            def _():
                down_copy_to(c, k).start()

            return 0

        lax.fori_loop(0, T, block_sum, 0)

    def stage_c(c):
        acc = xbuf[c, t].astype(jnp.float32) + down_out[c, 0].astype(jnp.float32)
        for k in range(1, T):
            down_copy_to(c, k).wait_recv()
            acc = acc + down_in[c, k].astype(jnp.float32)
        done_buf[c] = acc.astype(jnp.bfloat16)

        @pl.when(jnp.logical_not(last))
        def _():
            for k in range(T):
                pass_on(c, k).start()

        @pl.when(last)
        def _():
            for g in range(group):
                for replica in range(R):
                    section, local = final_copy(c, g, replica, "local")
                    _, remote = final_copy(c, g, replica, "remote")
                    mine = is_self(section, replica)

                    @pl.when(mine)
                    def _():
                        local.start()

                    @pl.when(jnp.logical_not(mine))
                    def _():
                        remote.start()

    early = 2 * s
    for p in range(len(moves)):

        @pl.when((s > failed) | ((s < failed) & (p < early)))
        def _():
            relay_piece(p)

    def step(i, _):
        @pl.when(i == 0)
        def _():
            weights_ready(0)

        @pl.when(i == 1)
        def _():
            weights_ready(1)

        @pl.when(i < chunks)
        def _():
            stage_a(i)

        @pl.when((i >= 1) & (i < chunks + 1))
        def _():
            stage_b(i - 1)

        @pl.when(i >= 2)
        def _():
            stage_c(i - 2)

        for p in range(len(moves)):

            @pl.when((s < failed) & (i + early == p))
            def _():
                relay_piece(p)

        return 0

    lax.fori_loop(0, chunks + 2, step, 0)
    for p in range(len(moves)):

        @pl.when((s < failed) & (p >= early + chunks + 2))
        def _():
            relay_piece(p)

    for slot in range(per_section):
        runs = s * per_section + slot < chunks * group

        @pl.when(runs)
        def _():
            for half in range(R):
                pltpu.make_async_copy(
                    done_buf.at[0, pl.ds(0, tok), :], fin.at[slot, half], fin_recv.at[slot, half]
                ).wait()
                finals_ref[slot, :, pl.ds(half * width, width)] = fin[slot, half]

        @pl.when(jnp.logical_not(runs))
        def _():
            finals_ref[slot] = jnp.zeros(finals_ref.shape[1:], finals_ref.dtype)

    @pl.when(is_failed)
    def _():
        for matrix, k in moves:
            spread(matrix, k, True).wait_send()

    @pl.when(jnp.logical_not(is_failed))
    def _():
        for matrix in range(2):
            forward(matrix, 0).wait_send()
        for matrix, k in moves:
            spread(matrix, k, False).wait_send()
            forward(matrix, k).wait_send()

    @pl.when(first)
    def _():
        for target in range(T):
            for block in range(R):

                @pl.when(jnp.logical_not((target == t) & (owner == d)))
                def _():
                    entering(block, target, "remote").wait_send()

    def drain(c, _):
        square_copy(c).wait_send()
        part_copy(c).wait_send()
        for k in range(1, T):
            down_copy_to(c, k).wait_send()

        @pl.when(jnp.logical_not(last))
        def _():
            for k in range(T):
                pass_on(c, k).wait_send()

        @pl.when(last)
        def _():
            for g in range(group):
                for replica in range(R):
                    section, remote = final_copy(c, g, replica, "remote")

                    @pl.when(jnp.logical_not(is_self(section, replica)))
                    def _():
                        remote.wait_send()

        return 0

    lax.fori_loop(0, chunks, drain, 0)


def relay(entering, gain, up, down, spare_up, spare_down, S, T, R, chunks, failed):
    batches, tok, share = entering.shape
    group = 1
    rows = group * R * tok
    width = share // R
    wide = up.shape[1]
    bf16, f32 = jnp.bfloat16, jnp.float32
    dma = pltpu.SemaphoreType.DMA
    vmem = pl.BlockSpec(memory_space=pltpu.VMEM)
    hbm = pl.BlockSpec(memory_space=pl.ANY)
    return pl.pallas_call(
        functools.partial(relay_kernel, (S, T, R, chunks, group, tok), failed),
        out_shape=jax.ShapeDtypeStruct((batches // S, tok, share), bf16),
        in_specs=[vmem, vmem, hbm, hbm, hbm, hbm],
        out_specs=vmem,
        scratch_shapes=[
            pltpu.VMEM(up.shape, bf16),
            pltpu.VMEM(down.shape, bf16),
            pltpu.VMEM((chunks, T, rows, width), bf16),
            pltpu.VMEM((chunks, rows, wide), bf16),
            pltpu.VMEM((chunks, rows, wide), bf16),
            pltpu.VMEM((chunks, rows, 128), f32),
            pltpu.VMEM((chunks, rows, 128), f32),
            pltpu.VMEM((chunks, T, rows, width), bf16),
            pltpu.VMEM((chunks, T, rows, width), bf16),
            pltpu.VMEM((chunks, rows, width), bf16),
            pltpu.VMEM((batches // S, R, tok, width), bf16),
            pltpu.VMEM((2, T, spare_up.shape[0], wide), bf16),
            dma((2,)),
            dma((2, T)),
            dma((2, T)),
            dma((2, T)),
            dma((2, S * T)),
            dma((R, T)),
            dma((T, R)),
            dma((chunks, T)),
            dma((chunks, T)),
            dma((chunks,)),
            dma((chunks,)),
            dma((chunks,)),
            dma((chunks,)),
            dma((chunks, T)),
            dma((chunks, T)),
            dma((batches, R)),
            dma((batches // S, R)),
        ],
        compiler_params=pltpu.CompilerParams(has_side_effects=True, vmem_limit_bytes=60 * 1024 * 1024),
    )(entering, gain, up, down, spare_up, spare_down)


SLOTS = (
    dict(
        FE=(4, 4, 4, 4),
        FD=(3, 3, 3, 3),
        C=(8, 7, 9, 15),
        FC=(2, 2, 2, 2),
        B=(6, 6, 8, 13),
        FG=(4, 4, 4, 4),
        FA=(0, 0, 0, 0),
        FB=(1, 1, 1, 1),
        A=(6, 5, 7, 12),
    ),
    dict(
        FC=(8, 8, 8, 7),
        FE=(12, 11, 11, 11),
        A=(0, 5, 13, 15),
        FD=(9, 9, 9, 8),
        FB=(6, 6, 6, 6),
        FA=(3, 5, 4, 5),
        C=(1, 6, 17, 18),
        FG=(12, 12, 11, 11),
        B=(0, 6, 15, 16),
    ),
    dict(
        FD=(21, 26, 23, 18),
        FC=(12, 19, 14, 15),
        FE=(30, 30, 30, 25),
        C=(3, 12, 32, 44),
        FA=(9, 13, 9, 12),
        FG=(31, 33, 31, 32),
        A=(0, 9, 28, 35),
        FB=(10, 16, 10, 13),
        B=(1, 10, 38, 40),
    ),
    dict(
        B=(1, 5, 10, 14),
        A=(0, 4, 9, 15),
        FG=(19, 20, 20, 20),
        FB=(12, 12, 12, 12),
        C=(1, 5, 10, 16),
        FA=(11, 11, 11, 11),
        FC=(12, 12, 13, 12),
        FD=(14, 13, 14, 13),
        FE=(16, 18, 16, 14),
    ),
)
PARTS = 2
TURN = 128
SWITCH = 2


def shared_kernel(
    sizes,
    failed,
    inputs_ref,
    gain_ref,
    up_hbm,
    down_hbm,
    spare_up,
    spare_down,
    finals_ref,
    up,
    down,
    turned,
    xbuf,
    part_out,
    part_in,
    square_out,
    square_in,
    down_out,
    down_in,
    done_buf,
    fin,
    f_up,
    f_down,
    f_gain,
    f_x,
    f_part,
    f_cross_in,
    f_line_out,
    f_line_in,
    f_hid,
    f_out,
    f_in,
    f_done,
    weight_sem,
    swap_send,
    swap_recv,
    gain_send,
    gain_recv,
    start_send,
    x_send,
    x_recv,
    part_send,
    part_recv,
    square_send,
    square_recv,
    down_send,
    down_recv,
    fin_send,
    fin_recv,
    fx_recv,
    cross_send,
    cross_recv,
    line_send,
    line_recv,
    hid_line_send,
    hid_line_recv,
    hid_cross_send,
    hid_cross_recv,
    leave_send,
    share_send,
    share_recv,
):
    S, T, R, G, chunks, tok = sizes
    s, t, d = lax.axis_index("section"), lax.axis_index("tensor"), lax.axis_index("dp")
    rows = R * tok
    width = xbuf.shape[-1]
    model = width * T * R
    wide = up.shape[1]
    piece = spare_up.shape[0]
    cols = f_up.shape[2]
    groups = S // G * R
    quarter = cols // groups
    block = wide // PARTS
    strip = rows // T
    per_section = finals_ref.shape[0]
    bf16, f32 = jnp.bfloat16, jnp.float32
    member, cluster = lax.rem(s, G), s // G
    mine = cluster * R + d
    is_failed, not_failed = s == failed, s != failed
    last_failed, first_failed = failed == S - 1, failed == 0

    up_copy = pltpu.make_async_copy(up_hbm, up, weight_sem.at[0])
    down_copy = pltpu.make_async_copy(down_hbm, down, weight_sem.at[1])

    def remote(src, dst, send, recv, where):
        return pltpu.make_async_remote_copy(src, dst, send, recv, device_id=where, device_id_type=MESH)

    def route(src, dst, send, recv, where):
        return where, lambda: pltpu.make_async_copy(src, dst, recv), lambda: remote(src, dst, send, recv, where)

    def is_self(where):
        return (where[0] == s) & (where[1] == t) & (where[2] == d)

    def go(routed):
        where, local, far = routed
        here = is_self(where)

        @pl.when(here)
        def _():
            local().start()

        @pl.when(jnp.logical_not(here))
        def _():
            far().start()

    def sent(routed):
        where, _, far = routed

        @pl.when(jnp.logical_not(is_self(where)))
        def _():
            far().wait_send()

    def landed(ref, sem):
        pltpu.make_async_copy(ref, ref, sem).wait()

    def each(count, act):
        def one(i, _):
            act(i)
            return 0

        lax.fori_loop(0, count, one, 0)

    spares, shared_weights = (spare_up, spare_down), (f_up, f_down)

    def swap_src(matrix, target):
        return spares[matrix].at[:, pl.ds(pl.multiple_of(target * cols, cols), cols)]

    def swap_own(matrix):
        return pltpu.make_async_copy(
            swap_src(matrix, member), shared_weights[matrix].at[member], swap_recv.at[matrix]
        )

    def swap_far(matrix, k):
        target = lax.rem(member + k, G)
        return remote(
            swap_src(matrix, target), shared_weights[matrix].at[member],
            swap_send.at[matrix, k], swap_recv.at[matrix], (cluster * G + target, t, d),
        )

    def swap_ready(matrix):
        landed(shared_weights[matrix], swap_recv.at[matrix])

    def gain_route(i):
        target, m = i // G, lax.rem(i, G)
        start = d * (T * width) + (target // G * G + m) * width + t * piece
        src = gain_ref.at[:, pl.ds(pl.multiple_of(start, piece), piece)]
        return route(src, f_gain.at[m], gain_send.at[i], gain_recv.at[0], (target, t, d))

    owner = t // (T // R)

    def entering(c, i):
        target, block = i // R, lax.rem(i, R)
        slot = lax.rem(t, T // R) * R + block
        src = inputs_ref.at[c, :, pl.ds(pl.multiple_of(block * width, width), width)]
        dst = xbuf.at[c, slot, pl.ds(pl.multiple_of(d * tok, tok), tok), :]
        return route(src, dst, start_send.at[c, i], x_recv.at[c], (s, target, owner))

    def entering_spare(c, i):
        target, block = i // R, lax.rem(i, R)
        slot = lax.rem(t, T // R) * R + block
        src = inputs_ref.at[c, :, pl.ds(pl.multiple_of(block * width + target * piece, piece), piece)]
        dst = f_x.at[c, lax.rem(slot, G), pl.ds(pl.multiple_of(d * tok, tok), tok), :]
        return route(src, dst, start_send.at[c, i], fx_recv.at[c], (s, target, owner))

    enters = (cluster == lax.rem(t, T // R) * R // G) if first_failed else (s == 0)
    entry = entering_spare if first_failed else entering

    def enter(c):
        @pl.when(enters & (c < chunks))
        def _():
            each(T * R, lambda i: go(entry(c, i)))

    def pass_on(c, target):
        return remote(done_buf.at[c], xbuf.at[c, t], x_send.at[c, target], x_recv.at[c], (s + 1, target, d))

    def pass_spare(c, i):
        target, m = i // G, lax.rem(i, G)
        src = done_buf.at[c, :, pl.ds(pl.multiple_of(target * piece, piece), piece)]
        return route(
            src, f_x.at[c, lax.rem(t, G)], x_send.at[c, i], fx_recv.at[c], (t // G * G + m, target, d)
        )

    def leave_spare(c, target):
        dst = xbuf.at[c, s, :, pl.ds(pl.multiple_of(t * piece, piece), piece)]
        return route(f_done.at[c], dst, leave_send.at[c, target], x_recv.at[c], (failed + 1, target, d))

    def final_normal(c, replica):
        block = d * T + t
        dst = fin.at[lax.rem(c, per_section), :, pl.ds(pl.multiple_of(lax.rem(block, R) * width, width), width)]
        return route(
            done_buf.at[c, pl.ds(replica * tok, tok), :], dst, fin_send.at[c, replica],
            fin_recv.at[lax.rem(c, per_section)], (c // per_section, block // R, replica),
        )

    def final_spare(c, replica):
        block = d * T + s
        start = pl.multiple_of(lax.rem(block, R) * width + t * piece, piece)
        return route(
            f_done.at[c, pl.ds(replica * tok, tok), :], fin.at[lax.rem(c, per_section), :, pl.ds(start, piece)],
            fin_send.at[c, replica], fin_recv.at[lax.rem(c, per_section)], (c // per_section, block // R, replica),
        )

    def part_copy(c, j):
        return remote(part_out.at[c, j], part_in.at[c, j], part_send.at[c, j], part_recv.at[c], (s, t, 1 - d))

    def square_copy(c):
        return remote(square_out.at[c], square_in.at[c], square_send.at[c], square_recv.at[c], (s, t, 1 - d))

    def down_copy_to(c, target):
        slot = lax.rem(target + T - t, T) - 1
        return remote(down_out.at[c, target], down_in.at[c, slot], down_send.at[c, target], down_recv.at[c], (s, target, d))

    def square_block(total):
        coarse = total.astype(bf16).astype(f32)
        lane = lax.broadcasted_iota(jnp.int32, (total.shape[0], 128), 1)
        return jnp.where(lane < 64, coarse, total - coarse).astype(bf16)

    def square_of(block):
        return block[:, 0:1] + block[:, 64:65]

    def stage_a(c):
        landed(xbuf.at[c], x_recv.at[c])
        total = jnp.zeros((rows, 1), f32)
        pieces = []
        for slot in range(T):
            values = xbuf[c, slot].astype(f32)
            total = total + jnp.sum(values * values, axis=1, keepdims=True)
            gain = gain_ref[:, pl.ds(slot * width, width)]
            for other in range(1, R):
                gain = jnp.where(d == other, gain_ref[:, pl.ds((other * T + slot) * width, width)], gain)
            pieces.append((values * gain).astype(bf16))
        square_out[c] = square_block(total)
        square_copy(c).start()
        scaled = jnp.concatenate(pieces, axis=1)

        def block_product(j):
            weights = up[:, pl.ds(pl.multiple_of(j * block, block), block)]
            part_out[c, j] = jnp.dot(scaled, weights, preferred_element_type=f32).astype(bf16)
            part_copy(c, j).start()

        each(PARTS, block_product)
        if not first_failed:
            enter(c + 1)

    def turn_down():
        down_copy.wait()

        def turn(i):
            at = pl.ds(pl.multiple_of(i // PARTS * TURN, TURN), TURN)
            side = pl.ds(pl.multiple_of(lax.rem(i, PARTS) * block, block), block)
            turned[side, at] = down[at, side].T

        each(down.shape[0] // TURN * PARTS, turn)

    def stage_b(c):
        landed(square_in.at[c], square_recv.at[c])
        landed(part_in.at[c], part_recv.at[c])
        squares = square_of(square_out[c].astype(f32) + square_in[c].astype(f32))
        scale = lax.rsqrt(squares * (1.0 / model) + 1e-05)
        pieces = []
        for j in range(PARTS):
            pre = (part_out[c, j].astype(f32) + part_in[c, j].astype(f32)) * scale
            pieces.append((pre / (1.0 + jnp.exp(-pre))).astype(bf16))
        hidden = jnp.concatenate(pieces, axis=1)

        def block_sum(i, _):
            target = jnp.where(t < T // 2, T - 1 - i, i)
            block = turned[:, pl.ds(pl.multiple_of(target * width, width), width)]
            down_out[c, target] = jnp.dot(hidden, block, preferred_element_type=f32).astype(bf16)

            @pl.when(target != t)
            def _():
                down_copy_to(c, target).start()

            return 0

        lax.fori_loop(0, T, block_sum, 0)

    def stage_c(c):
        landed(down_in.at[c], down_recv.at[c])
        acc = xbuf[c, t].astype(f32) + down_out[c, t].astype(f32)
        for k in range(T - 1):
            acc = acc + down_in[c, k].astype(f32)
        done_buf[c] = acc.astype(bf16)
        each_next(c, go, lambda copy: copy.start())

    def each_next(c, act, act_remote):
        if failed > 0:

            @pl.when(s == failed - 1)
            def _():
                each(T * G, lambda i: act(pass_spare(c, i)))

        @pl.when((s != failed - 1) & (s < S - 1))
        def _():
            each(T, lambda i: act_remote(pass_on(c, i)))

        if not last_failed:

            @pl.when(s == S - 1)
            def _():
                each(R, lambda i: act(final_normal(c, i)))

    def each_after(c, act):
        if last_failed:
            each(R, lambda i: act(final_spare(c, i)))
        else:
            each(T, lambda i: act(leave_spare(c, i)))

    def other_group(k):
        return lax.rem(mine + k, groups)

    def group_device(g, line):
        return (g // R * G + member, line, lax.rem(g, R))

    def cross_copy(c, k):
        g = other_group(k)
        return remote(
            f_part.at[c, g], f_cross_in.at[c, k - 1], cross_send.at[c, k], cross_recv.at[c], group_device(g, t)
        )

    def line_copy(c, k):
        target = lax.rem(t + k, T)
        src = f_line_out.at[c, pl.ds(pl.multiple_of(target * strip, strip), strip), :]
        return remote(src, f_line_in.at[c, k - 1], line_send.at[c, k], line_recv.at[c], (s, target, d))

    def hid_at(c, line):
        return f_hid.at[c, mine, pl.ds(pl.multiple_of(line * strip, strip), strip), :]

    def hid_line_copy(c, k):
        target = lax.rem(t + k, T)
        return remote(hid_at(c, t), hid_at(c, t), hid_line_send.at[c, k], hid_line_recv.at[c, t], (s, target, d))

    def hid_cross_copy(c, k, line):
        where = group_device(other_group(k), t)
        return remote(
            hid_at(c, line), hid_at(c, line), hid_cross_send.at[c, k * T + line], hid_cross_recv.at[c, mine], where
        )

    def share_copy(c, k):
        target = lax.rem(member + k, G)
        return remote(
            f_out.at[c, target], f_in.at[c, k - 1], share_send.at[c, k], share_recv.at[c], (cluster * G + target, t, d)
        )

    def spare_a(c):
        landed(f_x.at[c], fx_recv.at[c])
        values = jnp.concatenate([f_x[c, m] for m in range(G)], axis=1).astype(f32)
        squares = square_block(jnp.sum(values * values, axis=1, keepdims=True))
        gain = jnp.concatenate([f_gain[m] for m in range(G)], axis=1)
        scaled = (values * gain).astype(bf16)

        def group_product(i):
            g = other_group(i + 1)
            weights = f_up[:, :, pl.ds(pl.multiple_of(g * quarter, quarter), quarter)].reshape(G * piece, quarter)
            product = jnp.dot(scaled, weights, preferred_element_type=f32).astype(bf16)
            f_part[c, g, :, pl.ds(0, quarter)] = product
            f_part[c, g, :, pl.ds(quarter, 128)] = squares

            @pl.when(i < groups - 1)
            def _():
                cross_copy(c, i + 1).start()

        each(groups, group_product)
        if first_failed:
            enter(c + 1)

    def spare_b(c):
        landed(f_cross_in.at[c], cross_recv.at[c])
        total = f_part[c, mine].astype(f32)
        for k in range(groups - 1):
            total = total + f_cross_in[c, k].astype(f32)
        f_line_out[c, :, pl.ds(0, quarter)] = total[:, :quarter].astype(bf16)
        f_line_out[c, :, pl.ds(quarter, 128)] = square_block(square_of(total[:, quarter:]))
        each(T - 1, lambda i: line_copy(c, i + 1).start())

    def spare_c(c):
        landed(f_line_in.at[c], line_recv.at[c])
        at = pl.ds(pl.multiple_of(t * strip, strip), strip)
        total = f_line_out[c, at, :].astype(f32)
        for k in range(T - 1):
            total = total + f_line_in[c, k].astype(f32)
        mean_square = square_of(total[:, quarter:]) * (1.0 / model)
        pre = total[:, :quarter] * lax.rsqrt(mean_square + 1e-05)
        f_hid[c, mine, at, :] = (pre / (1.0 + jnp.exp(-pre))).astype(bf16)
        each(T - 1, lambda i: hid_line_copy(c, i + 1).start())
        each(groups - 1, lambda i: hid_cross_copy(c, i + 1, t).start())

    def spare_d(c):
        def forward(j):
            line = lax.rem(t + j + 1, T)
            landed(hid_at(c, line), hid_line_recv.at[c, line])
            each(groups - 1, lambda i: hid_cross_copy(c, i + 1, line).start())

        each(T - 1, forward)

    def spare_e(c):
        def arrived(i):
            g = other_group(i + 1)
            landed(f_hid.at[c, g], hid_cross_recv.at[c, g])

        each(groups - 1, arrived)
        hidden = jnp.concatenate([f_hid[c, g] for g in range(groups)], axis=1)
        weights = f_down[...].reshape(G * piece, cols)
        result = lax.dot_general(hidden, weights, (((1,), (1,)), ((), ())), preferred_element_type=f32)
        for m in range(G):
            f_out[c, m] = result[:, m * piece : (m + 1) * piece].astype(bf16)
        each(G - 1, lambda i: share_copy(c, i + 1).start())

    def spare_g(c):
        landed(f_in.at[c], share_recv.at[c])
        acc = f_x[c, member].astype(f32) + f_out[c, member].astype(f32)
        for k in range(G - 1):
            acc = acc + f_in[c, k].astype(f32)
        f_done[c] = acc.astype(bf16)
        each_after(c, go)

    @pl.when(not_failed)
    def _():
        up_copy.start()
        down_copy.start()

    for matrix in range(2):
        swap_own(matrix).start()
    barrier = pltpu.get_barrier_semaphore()

    def greet(i):
        where = (i // (T * R), lax.rem(i // R, T), lax.rem(i, R))

        @pl.when(jnp.logical_not(is_self(where)))
        def _():
            pl.semaphore_signal(barrier, inc=1, device_id=where, device_id_type=MESH)

    each(S * T * R, greet)
    pl.semaphore_wait(barrier, S * T * R - 1)
    enter(0)

    @pl.when(is_failed)
    def _():
        each(S * G, lambda i: go(gain_route(i)))

    for matrix in range(2):
        each(G - 1, lambda i: swap_far(matrix, i + 1).start())

    table = SLOTS[failed]

    def slot_of(task):
        offset = table[task][S - 1]
        for other in range(S - 1):
            offset = jnp.where(s == other, table[task][other], offset)
        return offset

    slots = {task: slot_of(task) + 1 for task in table}
    steps = max(max(row) for row in table.values()) + chunks + 1

    turn_slot = jnp.where(s == 0, slots["A"], 0)

    def step(i, _):
        def at(offset, allowed, stage):
            due = (i >= offset) & (i < offset + chunks)
            c = lax.rem(i + chunks * steps - offset, chunks)

            @pl.when(due if allowed is None else due & allowed)
            def _():
                stage(c)

        def first_time(c, ready):
            @pl.when(c == 0)
            def _():
                ready()

        def a(c):
            first_time(c, up_copy.wait)
            stage_a(c)

        def fa(c):
            def ready():
                swap_ready(0)
                landed(f_gain, gain_recv.at[0])

            first_time(c, ready)
            spare_a(c)

        def fe(c):
            first_time(c, lambda: swap_ready(1))
            spare_e(c)

        stages = dict(
            A=(not_failed, a), B=(not_failed, stage_b), C=(not_failed, stage_c), FA=(None, fa), FB=(None, spare_b),
            FC=(None, spare_c), FD=(None, spare_d), FE=(None, fe), FG=(None, spare_g),
        )
        for task in table:
            at(slots[task], *stages[task])
            if task == "A":

                @pl.when(not_failed & (i == turn_slot))
                def _():
                    turn_down()

        return 0

    lax.fori_loop(0, steps, step, 0)

    for matrix in range(2):
        each(G - 1, lambda i: swap_far(matrix, i + 1).wait_send())

    @pl.when(is_failed)
    def _():
        each(S * G, lambda i: sent(gain_route(i)))

    def drain(c):
        @pl.when(enters)
        def _():
            each(T * R, lambda i: sent(entry(c, i)))

        @pl.when(not_failed)
        def _():
            square_copy(c).wait_send()
            each(PARTS, lambda j: part_copy(c, j).wait_send())

            def one(target):
                @pl.when(target != t)
                def _():
                    down_copy_to(c, target).wait_send()

            each(T, one)
            each_next(c, sent, lambda copy: copy.wait_send())

        def group_sent(i):
            cross_copy(c, i + 1).wait_send()
            each(T, lambda line: hid_cross_copy(c, i + 1, line).wait_send())

        def line_sent(i):
            line_copy(c, i + 1).wait_send()
            hid_line_copy(c, i + 1).wait_send()

        each(groups - 1, group_sent)
        each(T - 1, line_sent)
        each(G - 1, lambda i: share_copy(c, i + 1).wait_send())
        each_after(c, sent)

    each(chunks, drain)

    for slot in range(per_section):
        runs = s * per_section + slot < chunks

        @pl.when(runs)
        def _():
            landed(fin.at[slot], fin_recv.at[slot])
            finals_ref[slot] = fin[slot]

        @pl.when(jnp.logical_not(runs))
        def _():
            finals_ref[slot] = jnp.zeros(finals_ref.shape[1:], finals_ref.dtype)


def shared(entering, gain, up, down, spare_up, spare_down, S, T, R, chunks, failed):
    batches, tok, share = entering.shape
    rows = R * tok
    width = share // R
    wide = up.shape[1]
    piece = spare_up.shape[0]
    G = S if failed >= SWITCH else 2
    cols = spare_up.shape[1] // G
    groups = S // G * R
    quarter = cols // groups
    block = wide // PARTS
    strip = rows // T
    bf16, f32 = jnp.bfloat16, jnp.float32
    dma = pltpu.SemaphoreType.DMA
    vmem = pl.BlockSpec(memory_space=pltpu.VMEM)
    hbm = pl.BlockSpec(memory_space=pl.ANY)
    per_section = batches // S
    return pl.pallas_call(
        functools.partial(shared_kernel, (S, T, R, G, chunks, tok), failed),
        out_shape=jax.ShapeDtypeStruct((per_section, tok, share), bf16),
        in_specs=[vmem, vmem, hbm, hbm, hbm, hbm],
        out_specs=vmem,
        scratch_shapes=[
            pltpu.VMEM(up.shape, bf16),
            pltpu.VMEM(down.shape, bf16),
            pltpu.VMEM((down.shape[1], down.shape[0]), bf16),
            pltpu.VMEM((chunks, T, rows, width), bf16),
            pltpu.VMEM((chunks, PARTS, rows, block), bf16),
            pltpu.VMEM((chunks, PARTS, rows, block), bf16),
            pltpu.VMEM((chunks, rows, 128), bf16),
            pltpu.VMEM((chunks, rows, 128), bf16),
            pltpu.VMEM((chunks, T, rows, width), bf16),
            pltpu.VMEM((chunks, T - 1, rows, width), bf16),
            pltpu.VMEM((chunks, rows, width), bf16),
            pltpu.VMEM((per_section, tok, share), bf16),
            pltpu.VMEM((G, piece, cols), bf16),
            pltpu.VMEM((G, piece, cols), bf16),
            pltpu.VMEM((G, 1, piece), f32),
            pltpu.VMEM((chunks, G, rows, piece), bf16),
            pltpu.VMEM((chunks, groups, rows, quarter + 128), bf16),
            pltpu.VMEM((chunks, groups - 1, rows, quarter + 128), bf16),
            pltpu.VMEM((chunks, rows, quarter + 128), bf16),
            pltpu.VMEM((chunks, T - 1, strip, quarter + 128), bf16),
            pltpu.VMEM((chunks, groups, rows, quarter), bf16),
            pltpu.VMEM((chunks, G, rows, piece), bf16),
            pltpu.VMEM((chunks, G - 1, rows, piece), bf16),
            pltpu.VMEM((chunks, rows, piece), bf16),
            dma((2,)),
            dma((2, G)),
            dma((2,)),
            dma((S * G,)),
            dma((1,)),
            dma((chunks, T * R)),
            dma((chunks, T * G)),
            dma((chunks,)),
            dma((chunks, PARTS)),
            dma((chunks,)),
            dma((chunks,)),
            dma((chunks,)),
            dma((chunks, T)),
            dma((chunks,)),
            dma((chunks, R)),
            dma((per_section,)),
            dma((chunks,)),
            dma((chunks, groups)),
            dma((chunks,)),
            dma((chunks, T)),
            dma((chunks,)),
            dma((chunks, T)),
            dma((chunks, T)),
            dma((chunks, T * groups)),
            dma((chunks, groups)),
            dma((chunks, T)),
            dma((chunks, G)),
            dma((chunks,)),
        ],
        compiler_params=pltpu.CompilerParams(
            collective_id=(batches - chunks) * S + failed, has_side_effects=True, vmem_limit_bytes=60 * 1024 * 1024
        ),
    )(entering, gain, up, down, spare_up, spare_down)


def spreads(S, T, R, tok, share, piece, columns, wide):
    width, rows = share // R, R * tok
    groups = S // 2 * R
    fits = S == len(SLOTS) and S == T and S % 2 == 0 and T % 2 == 0 and R == 2 and T // R * R == T and T // R == S // 2
    return fits and width == T * piece and T * width % TURN == 0 and piece % 128 == 0 and columns % (256 * groups) == 0 and wide % (128 * PARTS) == 0 and rows % (16 * T) == 0


def body(
    section_up,
    section_down,
    backup_up,
    backup_down,
    norm_gain,
    micro_batches,
    failed_section,
    live_batches,
):
    S, T, R = lax.axis_size("section"), lax.axis_size("tensor"), lax.axis_size("dp")
    batch_count, tok, share = micro_batches.shape
    live_count = batch_count // 2 + live_batches[0] % (batch_count - batch_count // 2 + 1)
    spare_up = backup_up.reshape(backup_up.shape[3:])
    spare_down = backup_down.reshape(backup_down.shape[3:])
    least = batch_count // 2
    stride = -(-(batch_count - least + 1) // 3)
    counts = list(range(batch_count, least - 1, -stride))
    chosen = (batch_count - live_count) // stride
    entering = micro_batches
    if stride > 1:
        alive = lax.broadcasted_iota(jnp.int32, (batch_count, 1, 1), 0) < live_count
        entering = jnp.where(alive, micro_batches, jnp.zeros_like(micro_batches))
    gain, call = norm_gain, shared
    if not spreads(S, T, R, tok, share, *spare_up.shape, section_up.shape[2]):
        depth = section_up.shape[1]
        gain = lax.dynamic_slice_in_dim(norm_gain, lax.axis_index("dp") * depth, depth, 1)
        call = relay
    operands = (entering, gain, section_up[0], section_down[0], spare_up, spare_down)

    def variant(failed, count):
        return lambda *arrays: call(*arrays, S, T, R, count, failed)

    variants = [variant(f, count) for count in counts for f in range(S)]
    return lax.switch(chosen * S + failed_section[0] % S, variants, *operands)


def solution(mesh):
    placed = (
        P("section", "dp", "tensor"),
        P("section", "dp", "tensor"),
        P("dp", "section", "tensor", None, None),
        P("dp", "section", "tensor", None, None),
        P("section", None),
        P(None, "dp", "tensor"),
        P(),
        P(),
    )
    return jax.shard_map(
        body, mesh=mesh, in_specs=placed, out_specs=P("section", "dp", "tensor"), check_vma=False
    )
```
